32 devices in a mesh: tm: 4 (over y, x), sky: 8 (over z, core).
Axes of the slice: x: 2, y: 2, z: 4, core: 2. Of those that a mesh axis runs over, the one named last changes fastest.
Arguments:
- residual: float32 [16384, 128], P(('tm', 'sky')), may hold values from -110 to 110
- obs_weight: float32 [16384, 128], P(('tm', 'sky')), may hold values from 0.5 to 2
- source_partials: float32 [5, 16384, 128], P(None, ('tm', 'sky')), may hold values from -1 to 1
- attitude_partials: float32 [16, 16384, 128], P(None, ('tm', 'sky')), may hold values from -1.5 to 1.5
- source_index: int32 [16384, 128], P(('tm', 'sky')), may hold values from 0 to 127
- tile_pixel: int32 [16384], P(('tm', 'sky')), may hold values from 0 to 1023, as said below
- tile_knot: int32 [16384], P(('tm', 'sky')), may hold values from 0 to 2047, as said below
- pixel_slot: int32 [1024], replicated, may hold values from 0 to 1023, as said below
Outputs:
- final_residual: float32 [16384, 128], P(('tm', 'sky'))
- source_update: float32 [5, 131072], P(None, 'sky')
- attitude_update: float32 [4, 2048], P(None, 'tm')
The draws below stay inside these ranges and needn't reach their ends.
Inputs may be any that keep to these rules, and one draw needn't show every extreme that they name: Tiles come in aligned blocks of 512; with owner = pixel_slot[tile_pixel[t]] // 128, no block holds more than 192 tiles of one owner, and every block holds exactly 192 tiles of some owner. `pixel_slot`: every slot number appears once. `tile_knot`: the tiles of aligned block q of 512 tiles have first knots in [q * 64, (q + 1) * 64).
All inputs are finite; a program needn't handle non-finite values.
Results may differ from the reference program's by a relative error of at most 0.0003.
Values sent between devices are 32-bit elements; how exact they have to be, the bound alone decides.
No kernel may reach another device: no remote copies, remote signals or barrier semaphores. Data moves between devices by JAX's collectives and lax.ppermute only.
A program may use at most 128 MiB of HBM per device.

```python
import math
import jax
import jax.numpy as jnp
from jax import lax

OBS_TILE = 128
TILES_DEV = 512
PIX_DEV = 128
SRC_PIX = 128
OWNERS = 8
TIME_SHARDS = 4
CAP = 192
SPAN = 64
PIXELS = 1024
KNOTS = 2048
TILES = 16384


def sky_layout(key):
    slot_of_pixel = jax.random.permutation(jax.random.fold_in(key, 11), PIXELS).astype(jnp.int32)
    pixel_of_slot = jnp.argsort(slot_of_pixel, stable=True).astype(jnp.int32)
    blocks = TILES // TILES_DEV
    crowded_rows = jax.random.randint(jax.random.fold_in(key, 12), (TIME_SHARDS,), 0, OWNERS)
    crowded = crowded_rows[jnp.arange(blocks, dtype=jnp.int32) // OWNERS]
    positions = jnp.arange(TILES_DEV, dtype=jnp.int32)
    remaining = positions - CAP
    plain_owner = (crowded[:, None] + 1 + remaining[None, :] % (OWNERS - 1)) % OWNERS
    owner_ids = jnp.where(positions[None, :] < CAP, crowded[:, None], plain_owner)
    shuffles = jax.vmap(lambda sub: jax.random.permutation(sub, TILES_DEV))(jax.random.split(jax.random.fold_in(key, 13), blocks))
    owner_ids = jnp.take_along_axis(owner_ids, shuffles, axis=1)
    local_pixel = jax.random.randint(jax.random.fold_in(key, 14), (blocks, TILES_DEV), 0, PIX_DEV)
    pixel_ids = pixel_of_slot[(owner_ids * PIX_DEV + local_pixel).reshape(-1)]
    return (slot_of_pixel, pixel_ids.astype(jnp.int32))


def draw_pixel_slot(key, part):
    return sky_layout(key)[0]


def draw_tile_pixel(key, part):
    return sky_layout(key)[1]


def knot_starts(key):
    offset = jax.random.randint(jax.random.fold_in(key, 21), (TILES,), 0, SPAN)
    return (jnp.arange(TILES, dtype=jnp.int32) // TILES_DEV * SPAN + offset).astype(jnp.int32)


def draw_tile_knot(key, part):
    return knot_starts(key)


def attitude_parts(key):
    partials = jnp.clip(0.25 * jax.random.normal(jax.random.fold_in(key, 31), (16, TILES, OBS_TILE), jnp.float32), -1.5, 1.5)
    return partials


def draw_attitude_partials(key, part):
    return attitude_parts(key)


def draw_residual(key, part):
    partials = attitude_parts(key)
    knot_start = knot_starts(key)
    attitude_curve = jnp.clip(jax.random.normal(jax.random.fold_in(key, 32), (4, KNOTS + 3), jnp.float32), -4.0, 4.0)
    signal = jnp.clip(jax.random.normal(jax.random.fold_in(key, 33), (TILES, OBS_TILE), jnp.float32), -6.0, 6.0)
    for segment in range(4):
        values = jnp.take(attitude_curve, knot_start + segment, axis=1)
        for component in range(4):
            signal = signal + partials[4 * segment + component] * values[component][:, None]
    return signal


def with_ends(values, rng, low, high):
    shape = values.shape
    spot = [jax.random.randint(jax.random.fold_in(rng, axis), (), 0, shape[axis]) for axis in range(len(shape))]
    values = values.at[tuple(spot)].set(low)
    longest = shape.index(max(shape))
    spot[longest] = (spot[longest] + 1) % shape[longest]
    return values.at[tuple(spot)].set(high)


def shard_levels(key, extent, cuts, low, top_value):
    gain, own = 1.0, jax.random.fold_in(key, 6)
    for axis_at, blocks in cuts:
        heights = jnp.exp(jax.random.uniform(jax.random.fold_in(own, axis_at), (blocks,), jnp.float32, low / len(cuts), top_value / len(cuts)))
        gain = gain * jnp.repeat(heights, extent[axis_at] // blocks).reshape([-1 if axis == axis_at else 1 for axis in range(len(extent))])
    return gain


def centred(own_key, extent, width, reach, cuts=(), kind=jnp.bfloat16):
    values = width * jax.random.normal(own_key, extent, jnp.float32)
    if cuts:
        values = values * shard_levels(own_key, extent, cuts, -0.22, 0.18)
    return jnp.clip(values, -reach, reach).astype(kind)


def setup_inputs(seed: int = 0) -> dict:
    arg_keys = jax.random.split(jax.random.key(seed), 9)
    return {
        "residual": draw_residual(jax.random.fold_in(arg_keys[8], 71), 0),
        "obs_weight": jnp.clip(jnp.exp(math.log(2.0) - 1.3862944 * jax.random.uniform(arg_keys[1], (TILES, OBS_TILE), jnp.float32) ** shard_levels(arg_keys[1], (TILES, OBS_TILE), ((0, 32),), -0.2, 0.2)), 0.5, 2.0),
        "source_partials": centred(arg_keys[2], (5, TILES, OBS_TILE), 32 ** -0.5, 1.0, ((1, 32),), jnp.float32),
        "attitude_partials": draw_attitude_partials(jax.random.fold_in(arg_keys[8], 71), 0),
        "source_index": with_ends(jax.random.randint(arg_keys[4], (TILES, OBS_TILE), 0, SRC_PIX), jax.random.fold_in(arg_keys[4], 1), 0, SRC_PIX - 1).astype(jnp.int32),
        "tile_pixel": draw_tile_pixel(jax.random.fold_in(arg_keys[8], 71), 0),
        "tile_knot": draw_tile_knot(jax.random.fold_in(arg_keys[8], 71), 0),
        "pixel_slot": draw_pixel_slot(jax.random.fold_in(arg_keys[8], 71), 0),
    }


SOURCE_PAIRS = tuple(((first, second) for first in range(5) for second in range(first, 5)))
KNOT_PAIRS = tuple(((first, second) for first in range(4) for second in range(first, 4)))

def damped_solve(normal, target, order, pairs):
    entries = {}
    for number, couple in enumerate(pairs):
        entries[couple] = normal[number]
    factor = {}
    for column in range(order):
        pivot_value = entries[column, column] + 1.0
        for earlier in range(column):
            pivot_value = pivot_value - factor[column, earlier] * factor[column, earlier]
        pivot_value = jnp.sqrt(pivot_value)
        factor[column, column] = pivot_value
        for below in range(column + 1, order):
            current = entries[column, below]
            for earlier in range(column):
                current = current - factor[below, earlier] * factor[column, earlier]
            factor[below, column] = current / pivot_value
    forward = []
    for column in range(order):
        current = target[column]
        for earlier in range(column):
            current = current - factor[column, earlier] * forward[earlier]
        forward.append(current / factor[column, column])
    answer = [None] * order
    for column in reversed(range(order)):
        current = forward[column]
        for later in range(column + 1, order):
            current = current - factor[later, column] * answer[later]
        answer[column] = current / factor[column, column]
    return jnp.stack(answer)

def source_terms(weights, partials, baseline):
    products = [weights * partials[first] * partials[second] for first, second in SOURCE_PAIRS]
    products = products + [weights * partials[first] * baseline for first in range(5)]
    return products

def knot_terms(weights, partials, baseline):
    result = []
    for segment in range(4):
        portion = partials[4 * segment:4 * segment + 4]
        sums_rows = [lax.optimization_barrier(jnp.sum(weights * portion[first] * portion[second], axis=-1)) for first, second in KNOT_PAIRS]
        sums_rows = sums_rows + [lax.optimization_barrier(jnp.sum(weights * portion[first] * baseline, axis=-1)) for first in range(4)]
        result.append(jnp.stack(sums_rows))
    return result

def correct(baseline, partials, picked):
    accumulated = partials[0] * picked[0]
    for component in range(1, partials.shape[0]):
        accumulated = accumulated + partials[component] * picked[component]
    return baseline - accumulated

def knot_correct(baseline, partials, extended, knot_start):
    accumulated = None
    for segment in range(4):
        values = jnp.take(extended, knot_start + segment, axis=1)
        for component in range(4):
            addend = partials[4 * segment + component] * values[component][:, None]
            accumulated = addend if accumulated is None else accumulated + addend
    return baseline - accumulated

def reference(residual, obs_weight, source_partials, attitude_partials, source_index, tile_pixel, tile_knot, pixel_slot):
    blocks = residual.shape[0] // TILES_DEV
    sources = pixel_slot.shape[0] * SRC_PIX
    source_id = (jnp.take(pixel_slot, tile_pixel)[:, None] * SRC_PIX + source_index).astype(jnp.int32)

    def add_block(running, number):
        offset = (number * TILES_DEV).astype(jnp.int32)
        baseline = lax.dynamic_slice_in_dim(residual, offset, TILES_DEV, 0)
        weights = lax.dynamic_slice_in_dim(obs_weight, offset, TILES_DEV, 0)
        partials = lax.dynamic_slice_in_dim(source_partials, offset, TILES_DEV, 1)
        indices = lax.dynamic_slice_in_dim(source_id, offset, TILES_DEV, 0)
        stacked = jnp.stack(source_terms(weights, partials, baseline), axis=-1).reshape(-1, 20)
        return (running + jax.ops.segment_sum(stacked, indices.reshape(-1), num_segments=sources), None)
    normals, _ = lax.scan(add_block, jnp.zeros((sources, 20), jnp.float32), jnp.arange(blocks, dtype=jnp.int32))
    normals = normals.T
    source_update = damped_solve(normals[:15], normals[15:], 5, SOURCE_PAIRS)
    picked = jnp.take(source_update, source_id, axis=1)
    settled = correct(residual, source_partials, picked)
    knots = KNOTS
    accumulated = jnp.zeros((14, knots + 3), jnp.float32)
    for segment, tile_sums in enumerate(knot_terms(obs_weight, attitude_partials, settled)):
        accumulated = accumulated + jax.ops.segment_sum(tile_sums.T, tile_knot + segment, num_segments=knots + 3).T
    attitude_update = damped_solve(accumulated[:10, :knots], accumulated[10:, :knots], 4, KNOT_PAIRS)
    extended = jnp.concatenate([attitude_update, jnp.zeros((4, 3), jnp.float32)], axis=1)
    final_residual = knot_correct(settled, attitude_partials, extended, tile_knot)
    return (final_residual, source_update, attitude_update)
```

```python
import functools

import jax
import jax.numpy as jnp
from jax import lax
from jax.experimental import pallas as pl
from jax.experimental.pallas import tpu as pltpu
from jax.sharding import PartitionSpec as P

SRC_PIX = 128
KNOTS_DEV = 512
ROWS = 24
GROUP = 8


SOURCE_PAIRS = tuple(((first, second) for first in range(5) for second in range(first, 5)))
KNOT_PAIRS = tuple(((first, second) for first in range(4) for second in range(first, 4)))


def damped_solve(normal, target, order, pairs):
    entries = {}
    for number, couple in enumerate(pairs):
        entries[couple] = normal[number]
    factor = {}
    for column in range(order):
        pivot_value = entries[column, column] + 1.0
        for earlier in range(column):
            pivot_value = pivot_value - factor[column, earlier] * factor[column, earlier]
        pivot_value = jnp.sqrt(pivot_value)
        factor[column, column] = pivot_value
        for below in range(column + 1, order):
            current = entries[column, below]
            for earlier in range(column):
                current = current - factor[below, earlier] * factor[column, earlier]
            factor[below, column] = current / pivot_value
    forward = []
    for column in range(order):
        current = target[column]
        for earlier in range(column):
            current = current - factor[column, earlier] * forward[earlier]
        forward.append(current / factor[column, column])
    answer = [None] * order
    for column in reversed(range(order)):
        current = forward[column]
        for later in range(column + 1, order):
            current = current - factor[later, column] * answer[later]
        answer[column] = current / factor[column, column]
    return jnp.stack(answer)


def normals_kernel(
    slot_ref, pixel_ref, residual_ref, weight_ref, partial_ref, index_ref, out_ref, table, products,
    *, sky, times, share,
):
    tiles = residual_ref.shape[0]
    pixels = table.shape[0] // ROWS

    def clear(number, carry):
        start = pl.multiple_of(number * 8 * ROWS, 8)
        table[pl.ds(start, 8 * ROWS), :] = jnp.zeros((8 * ROWS, 128), jnp.float32)
        return carry

    lax.fori_loop(0, pixels // 8, clear, 0)
    products[...] = jnp.zeros(products.shape, jnp.float32)
    lanes = lax.broadcasted_iota(jnp.int32, (SRC_PIX, 128), 0)

    def add_group(group, carry):
        start = pl.multiple_of(group * GROUP, GROUP)
        rows = pl.ds(start, GROUP)
        weight = weight_ref[rows, :]
        baseline = residual_ref[rows, :]
        parts = [partial_ref[number, rows, :] for number in range(5)]
        scaled = [weight * part for part in parts]
        terms = [scaled[first] * parts[second] for first, second in SOURCE_PAIRS]
        terms = terms + [scaled[first] * baseline for first in range(5)]
        for number, term in enumerate(terms):
            products[pl.ds(number, GROUP, stride=ROWS), :] = term
        sums = []
        for tile in range(GROUP):
            full = products[pl.ds(tile * ROWS, ROWS), :]
            high = full.astype(jnp.bfloat16).astype(jnp.float32)
            both = jnp.concatenate([high, full - high], axis=0).astype(jnp.bfloat16)
            chosen = index_ref[pl.ds(start + tile, 1), :]
            hits = jnp.where(lanes == chosen, 1.0, 0.0).astype(jnp.bfloat16)
            spread = lax.dot_general(
                both, hits, (((1,), (1,)), ((), ())), preferred_element_type=jnp.float32
            )
            sums.append(spread[:ROWS] + spread[ROWS:])
        for tile in range(GROUP):
            slot = slot_ref[pixel_ref[start + tile]]
            place = pl.ds(pl.multiple_of(slot * ROWS, 8), ROWS)
            table[place, :] = table[place, :] + sums[tile]
        return carry

    lax.fori_loop(0, tiles // GROUP, add_group, 0)

    def compact(number, carry):
        groups = share // 8
        device = number // groups
        inner = number % groups
        base = (device % sky) * (share * times) + (device // sky) * share + inner * 8
        for row in range(20):
            out_ref[device, row, pl.ds(pl.multiple_of(inner * 8, 8), 8), :] = table[
                pl.ds(base * ROWS + row, 8, stride=ROWS), :
            ]
        return carry

    lax.fori_loop(0, pixels // 8, compact, 0)


def local_normals(residual, weight, partials, index, tile_pixel, pixel_slot, sky, times):
    pixels = pixel_slot.shape[0]
    share = pixels // (sky * times)
    smem = pl.BlockSpec(memory_space=pltpu.SMEM)
    vmem = pl.BlockSpec(memory_space=pltpu.VMEM)
    return pl.pallas_call(
        functools.partial(normals_kernel, sky=sky, times=times, share=share),
        out_shape=jax.ShapeDtypeStruct((sky * times, 20, share, 128), jnp.float32),
        in_specs=[smem, smem, vmem, vmem, vmem, vmem],
        out_specs=vmem,
        scratch_shapes=[
            pltpu.VMEM((pixels * ROWS, 128), jnp.float32),
            pltpu.VMEM((GROUP * ROWS, 128), jnp.float32),
        ],
        compiler_params=pltpu.CompilerParams(vmem_limit_bytes=60000 * 1024),
        name="local_normals",
    )(pixel_slot, tile_pixel, residual, weight, partials, index)


def pair_kernel(weight_ref, attitude_ref, out_ref):
    lane = lax.broadcasted_iota(jnp.int32, (GROUP, 128), 1)

    def add_group(group, carry):
        rows = pl.ds(pl.multiple_of(group * GROUP, GROUP), GROUP)
        weight = weight_ref[rows, :]
        result = jnp.zeros((GROUP, 128), jnp.float32)
        for segment in range(4):
            parts = [attitude_ref[4 * segment + number, rows, :] for number in range(4)]
            scaled = [weight * part for part in parts]
            for number, (first, second) in enumerate(KNOT_PAIRS):
                total = jnp.sum(scaled[first] * parts[second], axis=1, keepdims=True)
                result = jnp.where(lane == 16 * segment + number, total, result)
        out_ref[rows, :] = result
        return carry

    lax.fori_loop(0, weight_ref.shape[0] // GROUP, add_group, 0)


def settle_kernel(
    slot_ref, pixel_ref, residual_ref, weight_ref, partial_ref, index_ref, attitude_ref,
    pairs_ref, update_ref, settled_ref, out_ref, picked, *, sky, times, share,
):
    block = residual_ref.shape[0]
    first_tile = pl.program_id(0) * block
    lane = lax.broadcasted_iota(jnp.int32, (GROUP, 128), 1)

    def add_group(group, carry):
        start = pl.multiple_of(group * GROUP, GROUP)
        rows = pl.ds(start, GROUP)
        for tile in range(GROUP):
            slot = slot_ref[pixel_ref[first_tile + start + tile]]
            device = (slot // share) % times * sky + slot // (share * times)
            base = device * (5 * share) + slot % share
            for number in range(5):
                picked[pl.ds(number * GROUP + tile, 1), :] = update_ref[
                    pl.ds(base + number * share, 1), :
                ]
        index = index_ref[rows, :]
        total = None
        for number in range(5):
            values = jnp.take_along_axis(picked[pl.ds(number * GROUP, GROUP), :], index, axis=1)
            addend = partial_ref[number, rows, :] * values
            total = addend if total is None else total + addend
        settled = residual_ref[rows, :] - total
        settled_ref[rows, :] = settled
        scaled = weight_ref[rows, :] * settled
        result = pairs_ref[rows, :]
        for segment in range(4):
            for number in range(4):
                amount = jnp.sum(
                    scaled * attitude_ref[4 * segment + number, rows, :], axis=1, keepdims=True
                )
                result = jnp.where(lane == 16 * segment + 10 + number, amount, result)
        out_ref[rows, :] = result
        return carry

    lax.fori_loop(0, block // GROUP, add_group, 0)


def final_kernel(settled_ref, attitude_ref, values_ref, out_ref):
    def correct_group(group, carry):
        rows = pl.ds(pl.multiple_of(group * GROUP, GROUP), GROUP)
        values = values_ref[rows, :]
        total = attitude_ref[0, rows, :] * values[:, 0:1]
        for number in range(1, 16):
            total = total + attitude_ref[number, rows, :] * values[:, number : number + 1]
        out_ref[rows, :] = settled_ref[rows, :] - total
        return carry

    lax.fori_loop(0, settled_ref.shape[0] // GROUP, correct_group, 0)


def body(
    residual,
    obs_weight,
    source_partials,
    attitude_partials,
    source_index,
    tile_pixel,
    tile_knot,
    pixel_slot,
):
    sky = lax.axis_size("sky")
    times = lax.axis_size("tm")
    both = ("tm", "sky")
    devices = sky * times
    tiles = residual.shape[0]
    pixels = pixel_slot.shape[0]
    share = pixels // devices
    span = KNOTS_DEV // sky
    block = min(tiles, 128)
    steps = tiles // block
    smem = pl.BlockSpec(memory_space=pltpu.SMEM)
    flat = pl.BlockSpec((block, 128), lambda step: (step, 0))
    five = pl.BlockSpec((5, block, 128), lambda step: (0, step, 0))
    wide = pl.BlockSpec((16, block, 128), lambda step: (0, step, 0))
    flat_shape = jax.ShapeDtypeStruct((tiles, 128), jnp.float32)

    normals = local_normals(
        residual, obs_weight, source_partials, source_index, tile_pixel, pixel_slot, sky, times
    )
    summed = lax.psum_scatter(normals, both, scatter_dimension=0, tiled=True)[0]
    pairs = pl.pallas_call(
        pair_kernel,
        grid=(steps,),
        out_shape=flat_shape,
        in_specs=[flat, wide],
        out_specs=flat,
        cost_estimate=pl.CostEstimate(
            flops=400 * tiles * 128 * 40, bytes_accessed=18 * tiles * 512, transcendentals=0
        ),
        name="knot_pairs",
    )(obs_weight, attitude_partials)
    update = damped_solve(summed[:15], summed[15:], 5, SOURCE_PAIRS)
    everything = lax.all_gather(update[None], both, axis=0, tiled=True)
    mine = lax.dynamic_slice_in_dim(
        everything.reshape(times, sky, 5, share * SRC_PIX), lax.axis_index("sky"), 1, 1
    )
    source_update = mine[:, 0].transpose(1, 0, 2).reshape(5, times * share * SRC_PIX)
    settled, terms = pl.pallas_call(
        functools.partial(settle_kernel, sky=sky, times=times, share=share),
        grid=(steps,),
        out_shape=(flat_shape, flat_shape),
        in_specs=[
            smem, smem, flat, flat, five, flat, wide, flat,
            pl.BlockSpec((devices * 5 * share, 128), lambda step: (0, 0)),
        ],
        out_specs=(flat, flat),
        scratch_shapes=[pltpu.VMEM((5 * GROUP, 128), jnp.float32)],
        name="settle",
    )(
        pixel_slot, tile_pixel, residual, obs_weight, source_partials, source_index,
        attitude_partials, pairs, everything.reshape(devices * 5 * share, 128),
    )
    number = lax.axis_index(both)
    start = tile_knot - number * span
    hits = (start[:, None] == jnp.arange(span, dtype=jnp.int32)[None, :]).astype(jnp.float32)
    sums = lax.dot_general(
        terms, hits, (((0,), (0,)), ((), ())), precision=lax.Precision.HIGHEST
    )
    local = sum(
        jnp.pad(sums[16 * segment : 16 * segment + 16], ((0, 0), (segment, 3 - segment)))
        for segment in range(4)
    )
    onward = [(device, device + 1) for device in range(devices - 1)]
    back = [(device + 1, device) for device in range(devices - 1)]
    arriving = lax.ppermute(local[:, span:], both, onward)
    whole = local[:, :span] + jnp.pad(arriving, ((0, 0), (0, span - 3)))
    own = damped_solve(whole[:10], whole[10:14], 4, KNOT_PAIRS)
    following = lax.ppermute(own[:, :3], both, back)
    attitude_update = lax.all_gather(own, "sky", axis=1, tiled=True)
    extended = jnp.concatenate([own, following], axis=1)
    windows = jnp.concatenate([extended[:, segment : segment + span] for segment in range(4)])
    values = lax.dot_general(
        hits, windows, (((1,), (1,)), ((), ())), precision=lax.Precision.HIGHEST
    )
    final_residual = pl.pallas_call(
        final_kernel,
        grid=(steps,),
        out_shape=flat_shape,
        in_specs=[flat, wide, pl.BlockSpec((block, 16), lambda step: (step, 0))],
        out_specs=flat,
        name="final",
    )(settled, attitude_partials, values)
    return (final_residual, source_update, attitude_update)


def solution(mesh):
    in_specs = (
        P(("tm", "sky"), None),
        P(("tm", "sky"), None),
        P(None, ("tm", "sky"), None),
        P(None, ("tm", "sky"), None),
        P(("tm", "sky"), None),
        P(("tm", "sky")),
        P(("tm", "sky")),
        P(),
    )
    out_specs = (P(("tm", "sky"), None), P(None, "sky"), P(None, "tm"))
    return jax.shard_map(body, mesh=mesh, in_specs=in_specs, out_specs=out_specs, check_vma=False)
```

```python
import functools

import jax
import jax.numpy as jnp
from jax import lax
from jax.experimental import pallas as pl
from jax.experimental.pallas import tpu as pltpu
from jax.sharding import PartitionSpec as P

SRC_PIX = 128
KNOTS_DEV = 512
ROWS = 24
GROUP = 8


SOURCE_PAIRS = tuple(((first, second) for first in range(5) for second in range(first, 5)))
KNOT_PAIRS = tuple(((first, second) for first in range(4) for second in range(first, 4)))


def damped_solve(normal, target, order, pairs):
    entries = {}
    for number, couple in enumerate(pairs):
        entries[couple] = normal[number]
    factor = {}
    for column in range(order):
        pivot_value = entries[column, column] + 1.0
        for earlier in range(column):
            pivot_value = pivot_value - factor[column, earlier] * factor[column, earlier]
        pivot_value = jnp.sqrt(pivot_value)
        factor[column, column] = pivot_value
        for below in range(column + 1, order):
            current = entries[column, below]
            for earlier in range(column):
                current = current - factor[below, earlier] * factor[column, earlier]
            factor[below, column] = current / pivot_value
    forward = []
    for column in range(order):
        current = target[column]
        for earlier in range(column):
            current = current - factor[column, earlier] * forward[earlier]
        forward.append(current / factor[column, column])
    answer = [None] * order
    for column in reversed(range(order)):
        current = forward[column]
        for later in range(column + 1, order):
            current = current - factor[later, column] * answer[later]
        answer[column] = current / factor[column, column]
    return jnp.stack(answer)


def bits_of(count):
    return count.bit_length() - 1


def halving_orders(sky, times):
    low, high = bits_of(sky), bits_of(sky * times)
    far = list(range(low, high))
    near = list(range(1, low))
    return ([0] + far + near, [0] + far[::-1] + near)


def swapped(value, axes, bit, devices):
    return lax.ppermute(value, axes, [(device, device ^ (1 << bit)) for device in range(devices)])


def normals_kernel(
    me_ref, slot_ref, pixel_ref, residual_ref, weight_ref, partial_ref, index_ref, *rest,
    sky, times, share,
):
    outs, table, products = rest[:-2], rest[-2], rest[-1]

    tiles = residual_ref.shape[0]
    pixels = table.shape[0] // ROWS

    def clear(number, carry):
        start = pl.multiple_of(number * 8 * ROWS, 8)
        table[pl.ds(start, 8 * ROWS), :] = jnp.zeros((8 * ROWS, 128), jnp.float32)
        return carry

    lax.fori_loop(0, pixels // 8, clear, 0)
    products[...] = jnp.zeros(products.shape, jnp.float32)
    lanes = lax.broadcasted_iota(jnp.int32, (SRC_PIX, 128), 0)

    def add_group(group, carry):
        start = pl.multiple_of(group * GROUP, GROUP)
        rows = pl.ds(start, GROUP)
        weight = weight_ref[rows, :]
        baseline = residual_ref[rows, :]
        parts = [partial_ref[number, rows, :] for number in range(5)]
        scaled = [weight * part for part in parts]
        terms = [scaled[first] * parts[second] for first, second in SOURCE_PAIRS]
        terms = terms + [scaled[first] * baseline for first in range(5)]
        for number, term in enumerate(terms):
            products[pl.ds(number, GROUP, stride=ROWS), :] = term
        sums = []
        for tile in range(GROUP):
            full = products[pl.ds(tile * ROWS, ROWS), :]
            high = full.astype(jnp.bfloat16).astype(jnp.float32)
            both = jnp.concatenate([high, full - high], axis=0).astype(jnp.bfloat16)
            chosen = index_ref[pl.ds(start + tile, 1), :]
            hits = jnp.where(lanes == chosen, 1.0, 0.0).astype(jnp.bfloat16)
            spread = lax.dot_general(
                both, hits, (((1,), (1,)), ((), ())), preferred_element_type=jnp.float32
            )
            sums.append(spread[:ROWS] + spread[ROWS:])
        for tile in range(GROUP):
            slot = slot_ref[pixel_ref[start + tile]]
            place = pl.ds(pl.multiple_of(slot * ROWS, 8), ROWS)
            table[place, :] = table[place, :] + sums[tile]
        return carry

    lax.fori_loop(0, tiles // GROUP, add_group, 0)

    me = me_ref[0]
    orders = halving_orders(sky, times)
    half = sky * times // 2
    length = bits_of(sky * times)
    for number, out_ref in enumerate(outs):
        chunk, sent = number // 2, number % 2
        order = orders[chunk % 2]

        def compact(place, carry):
            device = me ^ (sent << order[0])
            for at in range(1, length):
                device = device ^ (((place >> (length - 1 - at)) & 1) << order[at])
            base = (device % sky) * (share * times) + (device // sky) * share + chunk * 8
            for row in range(20):
                out_ref[place, row] = table[pl.ds(base * ROWS + row, 8, stride=ROWS), :]
            return carry

        lax.fori_loop(0, half, compact, 0)


def local_normals(me, residual, weight, partials, index, tile_pixel, pixel_slot, sky, times):
    pixels = pixel_slot.shape[0]
    share = pixels // (sky * times)
    smem = pl.BlockSpec(memory_space=pltpu.SMEM)
    vmem = pl.BlockSpec(memory_space=pltpu.VMEM)
    return pl.pallas_call(
        functools.partial(normals_kernel, sky=sky, times=times, share=share),
        out_shape=[
            jax.ShapeDtypeStruct((sky * times // 2, 20, 8, 128), jnp.float32)
            for _ in range(share // 4)
        ],
        in_specs=[smem, smem, smem, vmem, vmem, vmem, vmem],
        out_specs=[vmem] * (share // 4),
        scratch_shapes=[
            pltpu.VMEM((pixels * ROWS, 128), jnp.float32),
            pltpu.VMEM((GROUP * ROWS, 128), jnp.float32),
        ],
        compiler_params=pltpu.CompilerParams(vmem_limit_bytes=60000 * 1024),
        name="local_normals",
    )(me, pixel_slot, tile_pixel, residual, weight, partials, index)


def pair_kernel(weight_ref, attitude_ref, out_ref):
    lane = lax.broadcasted_iota(jnp.int32, (GROUP, 128), 1)

    def add_group(group, carry):
        rows = pl.ds(pl.multiple_of(group * GROUP, GROUP), GROUP)
        weight = weight_ref[rows, :]
        result = jnp.zeros((GROUP, 128), jnp.float32)
        for segment in range(4):
            parts = [attitude_ref[4 * segment + number, rows, :] for number in range(4)]
            scaled = [weight * part for part in parts]
            for number, (first, second) in enumerate(KNOT_PAIRS):
                total = jnp.sum(scaled[first] * parts[second], axis=1, keepdims=True)
                result = jnp.where(lane == 16 * segment + number, total, result)
        out_ref[rows, :] = result
        return carry

    lax.fori_loop(0, weight_ref.shape[0] // GROUP, add_group, 0)


def settle_kernel(
    base_ref, pixel_ref, residual_ref, weight_ref, partial_ref, index_ref, attitude_ref,
    pairs_ref, update_ref, settled_ref, out_ref, picked, *, part,
):
    block = residual_ref.shape[0]
    first_tile = pl.program_id(0) * block
    lane = lax.broadcasted_iota(jnp.int32, (GROUP, 128), 1)

    def add_group(group, carry):
        start = pl.multiple_of(group * GROUP, GROUP)
        rows = pl.ds(start, GROUP)
        for tile in range(GROUP):
            base = base_ref[pixel_ref[first_tile + start + tile]]
            for number in range(5):
                picked[pl.ds(number * GROUP + tile, 1), :] = update_ref[
                    pl.ds(base + number * part, 1), :
                ]
        index = index_ref[rows, :]
        total = None
        for number in range(5):
            values = jnp.take_along_axis(picked[pl.ds(number * GROUP, GROUP), :], index, axis=1)
            addend = partial_ref[number, rows, :] * values
            total = addend if total is None else total + addend
        settled = residual_ref[rows, :] - total
        settled_ref[rows, :] = settled
        scaled = weight_ref[rows, :] * settled
        result = pairs_ref[rows, :]
        for segment in range(4):
            for number in range(4):
                amount = jnp.sum(
                    scaled * attitude_ref[4 * segment + number, rows, :], axis=1, keepdims=True
                )
                result = jnp.where(lane == 16 * segment + 10 + number, amount, result)
        out_ref[rows, :] = result
        return carry

    lax.fori_loop(0, block // GROUP, add_group, 0)


def final_kernel(settled_ref, attitude_ref, values_ref, out_ref):
    def correct_group(group, carry):
        rows = pl.ds(pl.multiple_of(group * GROUP, GROUP), GROUP)
        values = values_ref[rows, :]
        total = attitude_ref[0, rows, :] * values[:, 0:1]
        for number in range(1, 16):
            total = total + attitude_ref[number, rows, :] * values[:, number : number + 1]
        out_ref[rows, :] = settled_ref[rows, :] - total
        return carry

    lax.fori_loop(0, settled_ref.shape[0] // GROUP, correct_group, 0)


def body(
    residual,
    obs_weight,
    source_partials,
    attitude_partials,
    source_index,
    tile_pixel,
    tile_knot,
    pixel_slot,
):
    sky = lax.axis_size("sky")
    times = lax.axis_size("tm")
    both = ("tm", "sky")
    devices = sky * times
    tiles = residual.shape[0]
    pixels = pixel_slot.shape[0]
    share = pixels // devices
    span = KNOTS_DEV // sky
    block = min(tiles, 128)
    steps = tiles // block
    smem = pl.BlockSpec(memory_space=pltpu.SMEM)
    flat = pl.BlockSpec((block, 128), lambda step: (step, 0))
    five = pl.BlockSpec((5, block, 128), lambda step: (0, step, 0))
    wide = pl.BlockSpec((16, block, 128), lambda step: (0, step, 0))
    flat_shape = jax.ShapeDtypeStruct((tiles, 128), jnp.float32)

    me = lax.axis_index(both)
    orders = halving_orders(sky, times)
    normals = local_normals(
        me[None], residual, obs_weight, source_partials, source_index, tile_pixel, pixel_slot,
        sky, times,
    )
    keeps, sends = list(normals[0::2]), list(normals[1::2])
    for step in range(bits_of(devices)):
        for chunk in range(len(keeps)):
            bit = orders[chunk % 2][step]
            arrived = swapped(sends[chunk], both, bit, devices)
            rest = keeps[chunk].shape[0] // 2
            if rest:
                sends[chunk] = keeps[chunk][rest:] + arrived[rest:]
                keeps[chunk] = keeps[chunk][:rest] + arrived[:rest]
            else:
                keeps[chunk] = keeps[chunk] + arrived
    summed = jnp.concatenate([keep[0] for keep in keeps], axis=1)
    pairs = pl.pallas_call(
        pair_kernel,
        grid=(steps,),
        out_shape=flat_shape,
        in_specs=[flat, wide],
        out_specs=flat,
        cost_estimate=pl.CostEstimate(
            flops=400 * tiles * 128 * 40, bytes_accessed=18 * tiles * 512, transcendentals=0
        ),
        name="knot_pairs",
    )(obs_weight, attitude_partials)
    update = damped_solve(summed[:15], summed[15:], 5, SOURCE_PAIRS)
    part = share // 2
    widths = [order[:0:-1] + [0] for order in orders]
    halves = []
    for side, order in enumerate(widths):
        held = update[None, :, side * part : (side + 1) * part]
        for bit in order:
            held = jnp.concatenate([held, swapped(held, both, bit, devices)], axis=0)
        halves.append(held)
    everything = jnp.concatenate([held.reshape(-1, SRC_PIX) for held in halves], axis=0)

    def spot(relative, order):
        place = 0
        for at, bit in enumerate(order):
            place = place + (((relative >> bit) & 1) << at)
        return place

    relative = me ^ ((pixel_slot // share) % times * sky + pixel_slot // (share * times))
    within = pixel_slot % share
    bases = [
        (side * devices + spot(relative, order)) * (5 * part) + within % part
        for side, order in enumerate(widths)
    ]
    base = jnp.where(within < part, bases[0], bases[1])
    time = lax.axis_index("tm")
    near = jnp.stack(
        [
            jnp.concatenate(
                [halves[side][spot(step * sky, widths[side])] for side in range(2)], axis=1
            )
            for step in range(times)
        ]
    )
    source_update = jnp.concatenate(
        [
            lax.dynamic_index_in_dim(near, time ^ step, 0, keepdims=False)
            for step in range(times)
        ],
        axis=1,
    ).reshape(5, times * share * SRC_PIX)
    settled, terms = pl.pallas_call(
        functools.partial(settle_kernel, part=part),
        grid=(steps,),
        out_shape=(flat_shape, flat_shape),
        in_specs=[
            smem, smem, flat, flat, five, flat, wide, flat,
            pl.BlockSpec((devices * 5 * share, 128), lambda step: (0, 0)),
        ],
        out_specs=(flat, flat),
        scratch_shapes=[pltpu.VMEM((5 * GROUP, 128), jnp.float32)],
        name="settle",
    )(
        base, tile_pixel, residual, obs_weight, source_partials, source_index,
        attitude_partials, pairs, everything,
    )
    start = tile_knot - me * span
    hits = (start[:, None] == jnp.arange(span, dtype=jnp.int32)[None, :]).astype(jnp.float32)
    sums = lax.dot_general(
        terms, hits, (((0,), (0,)), ((), ())), precision=lax.Precision.HIGHEST
    )
    local = sum(
        jnp.pad(sums[16 * segment : 16 * segment + 16], ((0, 0), (segment, 3 - segment)))
        for segment in range(4)
    )
    onward = [(device, device + 1) for device in range(devices - 1)]
    back = [(device + 1, device) for device in range(devices - 1)]
    arriving = lax.ppermute(local[:, span:], both, onward)
    whole = local[:, :span] + jnp.pad(arriving, ((0, 0), (0, span - 3)))
    own = damped_solve(whole[:10], whole[10:14], 4, KNOT_PAIRS)
    following = lax.ppermute(own[:, :3], both, back)
    pieces = [own] + [
        lax.ppermute(own, "sky", [(device, device ^ step) for device in range(sky)])
        for step in range(1, sky)
    ]
    stacked = jnp.stack(pieces)
    order = jnp.arange(sky, dtype=jnp.int32)
    turn = (order[:, None] ^ lax.axis_index("sky") == order[None, :]).astype(jnp.float32)
    attitude_update = jnp.einsum(
        "jr,rck->cjk", turn, stacked, precision=lax.Precision.HIGHEST
    ).reshape(4, sky * span)
    extended = jnp.concatenate([own, following], axis=1)
    windows = jnp.concatenate([extended[:, segment : segment + span] for segment in range(4)])
    values = lax.dot_general(
        hits, windows, (((1,), (1,)), ((), ())), precision=lax.Precision.HIGHEST
    )
    final_residual = pl.pallas_call(
        final_kernel,
        grid=(steps,),
        out_shape=flat_shape,
        in_specs=[flat, wide, pl.BlockSpec((block, 16), lambda step: (step, 0))],
        out_specs=flat,
        name="final",
    )(settled, attitude_partials, values)
    return (final_residual, source_update, attitude_update)


def solution(mesh):
    in_specs = (
        P(("tm", "sky"), None),
        P(("tm", "sky"), None),
        P(None, ("tm", "sky"), None),
        P(None, ("tm", "sky"), None),
        P(("tm", "sky"), None),
        P(("tm", "sky")),
        P(("tm", "sky")),
        P(),
    )
    out_specs = (P(("tm", "sky"), None), P(None, "sky"), P(None, "tm"))
    return jax.shard_map(body, mesh=mesh, in_specs=in_specs, out_specs=out_specs, check_vma=False)
```

```python
import functools

import jax
import jax.numpy as jnp
from jax import lax
from jax.experimental import pallas as pl
from jax.experimental.pallas import tpu as pltpu
from jax.sharding import PartitionSpec as P

SRC_PIX = 128
KNOTS_DEV = 512
ROWS = 24
GROUP = 8


SOURCE_PAIRS = tuple(((first, second) for first in range(5) for second in range(first, 5)))
KNOT_PAIRS = tuple(((first, second) for first in range(4) for second in range(first, 4)))


def damped_solve(normal, target, order, pairs):
    entries = {}
    for number, couple in enumerate(pairs):
        entries[couple] = normal[number]
    factor = {}
    for column in range(order):
        pivot_value = entries[column, column] + 1.0
        for earlier in range(column):
            pivot_value = pivot_value - factor[column, earlier] * factor[column, earlier]
        pivot_value = jnp.sqrt(pivot_value)
        factor[column, column] = pivot_value
        for below in range(column + 1, order):
            current = entries[column, below]
            for earlier in range(column):
                current = current - factor[below, earlier] * factor[column, earlier]
            factor[below, column] = current / pivot_value
    forward = []
    for column in range(order):
        current = target[column]
        for earlier in range(column):
            current = current - factor[column, earlier] * forward[earlier]
        forward.append(current / factor[column, column])
    answer = [None] * order
    for column in reversed(range(order)):
        current = forward[column]
        for later in range(column + 1, order):
            current = current - factor[later, column] * answer[later]
        answer[column] = current / factor[column, column]
    return jnp.stack(answer)


def bits_of(count):
    return count.bit_length() - 1


def halving_orders(sky, times):
    low, high = bits_of(sky), bits_of(sky * times)
    far = list(range(low, high))
    near = list(range(1, low))
    return (
        [0] + far + near,
        [0] + far[::-1] + near,
        [0] + near + far,
        [0] + far[::-1] + near,
    )


def over_groups(count, unroll, one):
    unroll = unroll if count % unroll == 0 else 1

    def several(number, carry):
        for area in range(unroll):
            one(number * unroll + area, area)
        return carry

    lax.fori_loop(0, count // unroll, several, 0)


def swapped(value, axes, bit, devices):
    return lax.ppermute(value, axes, [(device, device ^ (1 << bit)) for device in range(devices)])


def normals_kernel(
    me_ref, slot_ref, pixel_ref, residual_ref, weight_ref, partial_ref, index_ref, *rest,
    sky, times, share,
):
    outs, table, products = rest[:-2], rest[-2], rest[-1]

    tiles = residual_ref.shape[0]
    pixels = table.shape[0] // ROWS

    def clear(number, carry):
        start = pl.multiple_of(number * 8 * ROWS, 8)
        table[pl.ds(start, 8 * ROWS), :] = jnp.zeros((8 * ROWS, 128), jnp.float32)
        return carry

    lax.fori_loop(0, pixels // 8, clear, 0)
    products[...] = jnp.zeros(products.shape, jnp.float32)
    lanes = lax.broadcasted_iota(jnp.int32, (SRC_PIX, 128), 0)

    def add_group(group, area):
        start = pl.multiple_of(group * GROUP, GROUP)
        rows = pl.ds(start, GROUP)
        weight = weight_ref[rows, :]
        baseline = residual_ref[rows, :]
        parts = [partial_ref[number, rows, :] for number in range(5)]
        scaled = [weight * part for part in parts]
        terms = [scaled[first] * parts[second] for first, second in SOURCE_PAIRS]
        terms = terms + [scaled[first] * baseline for first in range(5)]
        for number, term in enumerate(terms):
            products[pl.ds(area * GROUP * ROWS + number, GROUP, stride=ROWS), :] = term
        sums = []
        for tile in range(GROUP):
            full = products[pl.ds((area * GROUP + tile) * ROWS, ROWS), :]
            high = full.astype(jnp.bfloat16).astype(jnp.float32)
            both = jnp.concatenate([high, full - high], axis=0).astype(jnp.bfloat16)
            chosen = index_ref[pl.ds(start + tile, 1), :]
            hits = jnp.where(lanes == chosen, 1.0, 0.0).astype(jnp.bfloat16)
            spread = lax.dot_general(
                both, hits, (((1,), (1,)), ((), ())), preferred_element_type=jnp.float32
            )
            sums.append(spread[:ROWS] + spread[ROWS:])
        for tile in range(GROUP):
            slot = slot_ref[pixel_ref[start + tile]]
            place = pl.ds(pl.multiple_of(slot * ROWS, 8), ROWS)
            table[place, :] = table[place, :] + sums[tile]

    over_groups(tiles // GROUP, 2, add_group)

    me = me_ref[0]
    orders = halving_orders(sky, times)
    half = sky * times // 2
    length = bits_of(sky * times)
    for number, out_ref in enumerate(outs):
        chunk, sent = number // 2, number % 2
        order = orders[chunk % 4]

        def compact(place, carry):
            device = me ^ (sent << order[0])
            for at in range(1, length):
                device = device ^ (((place >> (length - 1 - at)) & 1) << order[at])
            base = (device % sky) * (share * times) + (device // sky) * share + chunk * 8
            for row in range(20):
                out_ref[place, row] = table[pl.ds(base * ROWS + row, 8, stride=ROWS), :]
            return carry

        lax.fori_loop(0, half, compact, 0)


def local_normals(me, residual, weight, partials, index, tile_pixel, pixel_slot, sky, times):
    pixels = pixel_slot.shape[0]
    share = pixels // (sky * times)
    smem = pl.BlockSpec(memory_space=pltpu.SMEM)
    vmem = pl.BlockSpec(memory_space=pltpu.VMEM)
    return pl.pallas_call(
        functools.partial(normals_kernel, sky=sky, times=times, share=share),
        out_shape=[
            jax.ShapeDtypeStruct((sky * times // 2, 20, 8, 128), jnp.float32)
            for _ in range(share // 4)
        ],
        in_specs=[smem, smem, smem, vmem, vmem, vmem, vmem],
        out_specs=[vmem] * (share // 4),
        scratch_shapes=[
            pltpu.VMEM((pixels * ROWS, 128), jnp.float32),
            pltpu.VMEM((2 * GROUP * ROWS, 128), jnp.float32),
        ],
        compiler_params=pltpu.CompilerParams(vmem_limit_bytes=60000 * 1024),
        name="local_normals",
    )(me, pixel_slot, tile_pixel, residual, weight, partials, index)


def pair_kernel(weight_ref, attitude_ref, out_ref):
    lane = lax.broadcasted_iota(jnp.int32, (GROUP, 128), 1)

    def add_group(group, area):
        rows = pl.ds(pl.multiple_of(group * GROUP, GROUP), GROUP)
        weight = weight_ref[rows, :]
        result = jnp.zeros((GROUP, 128), jnp.float32)
        for segment in range(4):
            parts = [attitude_ref[4 * segment + number, rows, :] for number in range(4)]
            scaled = [weight * part for part in parts]
            for number, (first, second) in enumerate(KNOT_PAIRS):
                total = jnp.sum(scaled[first] * parts[second], axis=1, keepdims=True)
                result = jnp.where(lane == 16 * segment + number, total, result)
        out_ref[rows, :] = result

    over_groups(weight_ref.shape[0] // GROUP, 4, add_group)


def settle_kernel(
    base_ref, pixel_ref, residual_ref, weight_ref, partial_ref, index_ref, attitude_ref,
    pairs_ref, update_ref, settled_ref, out_ref, picked, *, part,
):
    block = residual_ref.shape[0]
    first_tile = pl.program_id(0) * block
    lane = lax.broadcasted_iota(jnp.int32, (GROUP, 128), 1)

    def add_group(group, area):
        start = pl.multiple_of(group * GROUP, GROUP)
        rows = pl.ds(start, GROUP)
        for tile in range(GROUP):
            base = base_ref[pixel_ref[first_tile + start + tile]]
            for number in range(5):
                picked[pl.ds((area * 5 + number) * GROUP + tile, 1), :] = update_ref[
                    pl.ds(base + number * part, 1), :
                ]
        index = index_ref[rows, :]
        total = None
        for number in range(5):
            values = jnp.take_along_axis(picked[pl.ds((area * 5 + number) * GROUP, GROUP), :], index, axis=1)
            addend = partial_ref[number, rows, :] * values
            total = addend if total is None else total + addend
        settled = residual_ref[rows, :] - total
        settled_ref[rows, :] = settled
        scaled = weight_ref[rows, :] * settled
        result = pairs_ref[rows, :]
        for segment in range(4):
            for number in range(4):
                amount = jnp.sum(
                    scaled * attitude_ref[4 * segment + number, rows, :], axis=1, keepdims=True
                )
                result = jnp.where(lane == 16 * segment + 10 + number, amount, result)
        out_ref[rows, :] = result

    over_groups(block // GROUP, 4, add_group)


def final_kernel(settled_ref, attitude_ref, values_ref, out_ref):
    def correct_group(group, area):
        rows = pl.ds(pl.multiple_of(group * GROUP, GROUP), GROUP)
        values = values_ref[rows, :]
        total = attitude_ref[0, rows, :] * values[:, 0:1]
        for number in range(1, 16):
            total = total + attitude_ref[number, rows, :] * values[:, number : number + 1]
        out_ref[rows, :] = settled_ref[rows, :] - total

    over_groups(settled_ref.shape[0] // GROUP, 4, correct_group)


def body(
    residual,
    obs_weight,
    source_partials,
    attitude_partials,
    source_index,
    tile_pixel,
    tile_knot,
    pixel_slot,
):
    sky = lax.axis_size("sky")
    times = lax.axis_size("tm")
    both = ("tm", "sky")
    devices = sky * times
    tiles = residual.shape[0]
    pixels = pixel_slot.shape[0]
    share = pixels // devices
    span = KNOTS_DEV // sky
    block = min(tiles, 128)
    steps = tiles // block
    smem = pl.BlockSpec(memory_space=pltpu.SMEM)
    flat = pl.BlockSpec((block, 128), lambda step: (step, 0))
    five = pl.BlockSpec((5, block, 128), lambda step: (0, step, 0))
    wide = pl.BlockSpec((16, block, 128), lambda step: (0, step, 0))
    flat_shape = jax.ShapeDtypeStruct((tiles, 128), jnp.float32)

    me = lax.axis_index(both)
    orders = halving_orders(sky, times)
    normals = local_normals(
        me[None], residual, obs_weight, source_partials, source_index, tile_pixel, pixel_slot,
        sky, times,
    )
    keeps, sends = list(normals[0::2]), list(normals[1::2])
    for step in range(bits_of(devices)):
        for chunk in range(len(keeps)):
            bit = orders[chunk % 4][step]
            arrived = swapped(sends[chunk], both, bit, devices)
            rest = keeps[chunk].shape[0] // 2
            if rest:
                sends[chunk] = keeps[chunk][rest:] + arrived[rest:]
                keeps[chunk] = keeps[chunk][:rest] + arrived[:rest]
            else:
                keeps[chunk] = keeps[chunk] + arrived
    summed = jnp.concatenate([keep[0] for keep in keeps], axis=1)
    pairs = pl.pallas_call(
        pair_kernel,
        grid=(steps,),
        out_shape=flat_shape,
        in_specs=[flat, wide],
        out_specs=flat,
        cost_estimate=pl.CostEstimate(
            flops=400 * tiles * 128 * 40, bytes_accessed=18 * tiles * 512, transcendentals=0
        ),
        name="knot_pairs",
    )(obs_weight, attitude_partials)
    update = damped_solve(summed[:15], summed[15:], 5, SOURCE_PAIRS)
    part = share // 2
    widths = [order[:0:-1] + [0] for order in orders[:2]]
    halves = []
    for side, order in enumerate(widths):
        held = update[None, :, side * part : (side + 1) * part]
        for bit in order:
            held = jnp.concatenate([held, swapped(held, both, bit, devices)], axis=0)
        halves.append(held)
    everything = jnp.concatenate([held.reshape(-1, SRC_PIX) for held in halves], axis=0)

    def spot(relative, order):
        place = 0
        for at, bit in enumerate(order):
            place = place + (((relative >> bit) & 1) << at)
        return place

    relative = me ^ ((pixel_slot // share) % times * sky + pixel_slot // (share * times))
    within = pixel_slot % share
    bases = [
        (side * devices + spot(relative, order)) * (5 * part) + within % part
        for side, order in enumerate(widths)
    ]
    base = jnp.where(within < part, bases[0], bases[1])
    time = lax.axis_index("tm")
    near = jnp.stack(
        [
            jnp.concatenate(
                [halves[side][spot(step * sky, widths[side])] for side in range(2)], axis=1
            )
            for step in range(times)
        ]
    )
    source_update = jnp.concatenate(
        [
            lax.dynamic_index_in_dim(near, time ^ step, 0, keepdims=False)
            for step in range(times)
        ],
        axis=1,
    ).reshape(5, times * share * SRC_PIX)
    settled, terms = pl.pallas_call(
        functools.partial(settle_kernel, part=part),
        grid=(steps,),
        out_shape=(flat_shape, flat_shape),
        in_specs=[
            smem, smem, flat, flat, five, flat, wide, flat,
            pl.BlockSpec((devices * 5 * share, 128), lambda step: (0, 0)),
        ],
        out_specs=(flat, flat),
        scratch_shapes=[pltpu.VMEM((4 * 5 * GROUP, 128), jnp.float32)],
        name="settle",
    )(
        base, tile_pixel, residual, obs_weight, source_partials, source_index,
        attitude_partials, pairs, everything,
    )
    start = tile_knot - me * span
    hits = (start[:, None] == jnp.arange(span, dtype=jnp.int32)[None, :]).astype(jnp.float32)
    sums = lax.dot_general(
        terms, hits, (((0,), (0,)), ((), ())), precision=lax.Precision.HIGHEST
    )
    local = sum(
        jnp.pad(sums[16 * segment : 16 * segment + 16], ((0, 0), (segment, 3 - segment)))
        for segment in range(4)
    )
    onward = [(device, device + 1) for device in range(devices - 1)]
    back = [(device + 1, device) for device in range(devices - 1)]
    arriving = lax.ppermute(local[:, span:], both, onward)
    whole = local[:, :span] + jnp.pad(arriving, ((0, 0), (0, span - 3)))
    own = damped_solve(whole[:10], whole[10:14], 4, KNOT_PAIRS)
    following = lax.ppermute(own[:, :3], both, back)
    stacked = own[None]
    for bit in range(bits_of(sky)):
        stacked = jnp.concatenate([stacked, swapped(stacked, "sky", bit, sky)], axis=0)
    order = jnp.arange(sky, dtype=jnp.int32)
    turn = (order[:, None] ^ lax.axis_index("sky") == order[None, :]).astype(jnp.float32)
    attitude_update = jnp.einsum(
        "jr,rck->cjk", turn, stacked, precision=lax.Precision.HIGHEST
    ).reshape(4, sky * span)
    extended = jnp.concatenate([own, following], axis=1)
    windows = jnp.concatenate([extended[:, segment : segment + span] for segment in range(4)])
    values = lax.dot_general(
        hits, windows, (((1,), (1,)), ((), ())), precision=lax.Precision.HIGHEST
    )
    final_residual = pl.pallas_call(
        final_kernel,
        grid=(steps,),
        out_shape=flat_shape,
        in_specs=[flat, wide, pl.BlockSpec((block, 16), lambda step: (step, 0))],
        out_specs=flat,
        name="final",
    )(settled, attitude_partials, values)
    return (final_residual, source_update, attitude_update)


def solution(mesh):
    in_specs = (
        P(("tm", "sky"), None),
        P(("tm", "sky"), None),
        P(None, ("tm", "sky"), None),
        P(None, ("tm", "sky"), None),
        P(("tm", "sky"), None),
        P(("tm", "sky")),
        P(("tm", "sky")),
        P(),
    )
    out_specs = (P(("tm", "sky"), None), P(None, "sky"), P(None, "tm"))
    return jax.shard_map(body, mesh=mesh, in_specs=in_specs, out_specs=out_specs, check_vma=False)
```

```python
import functools

import jax
import jax.numpy as jnp
from jax import lax
from jax.experimental import pallas as pl
from jax.experimental.pallas import tpu as pltpu
from jax.sharding import PartitionSpec as P

SRC_PIX = 128
KNOTS_DEV = 512
ROWS = 24
GROUP = 8


SOURCE_PAIRS = tuple(((first, second) for first in range(5) for second in range(first, 5)))
KNOT_PAIRS = tuple(((first, second) for first in range(4) for second in range(first, 4)))


def damped_solve(normal, target, order, pairs):
    entries = {}
    for number, couple in enumerate(pairs):
        entries[couple] = normal[number]
    factor = {}
    for column in range(order):
        pivot_value = entries[column, column] + 1.0
        for earlier in range(column):
            pivot_value = pivot_value - factor[column, earlier] * factor[column, earlier]
        pivot_value = jnp.sqrt(pivot_value)
        factor[column, column] = pivot_value
        for below in range(column + 1, order):
            current = entries[column, below]
            for earlier in range(column):
                current = current - factor[below, earlier] * factor[column, earlier]
            factor[below, column] = current / pivot_value
    forward = []
    for column in range(order):
        current = target[column]
        for earlier in range(column):
            current = current - factor[column, earlier] * forward[earlier]
        forward.append(current / factor[column, column])
    answer = [None] * order
    for column in reversed(range(order)):
        current = forward[column]
        for later in range(column + 1, order):
            current = current - factor[later, column] * answer[later]
        answer[column] = current / factor[column, column]
    return jnp.stack(answer)


def bits_of(count):
    return count.bit_length() - 1


def halving_orders(sky, times):
    low, high = bits_of(sky), bits_of(sky * times)
    far = list(range(low, high))
    near = list(range(1, low))
    return (
        [0] + far + near,
        [0] + far[::-1] + near,
        [0] + near + far,
        [0] + far[::-1] + near,
    )


def over_groups(count, unroll, one):
    unroll = unroll if count % unroll == 0 else 1

    def several(number, carry):
        for area in range(unroll):
            one(number * unroll + area, area)
        return carry

    lax.fori_loop(0, count // unroll, several, 0)


def swapped(value, axes, bit, devices):
    return lax.ppermute(value, axes, [(device, device ^ (1 << bit)) for device in range(devices)])


def normals_kernel(
    me_ref, slot_ref, pixel_ref, residual_ref, weight_ref, partial_ref, index_ref, *rest,
    sky, times, share,
):
    count = (len(rest) - 3) // 2
    outs, stages = rest[:count], rest[count : 2 * count]
    table, products, done = rest[2 * count :]
    copies = []

    tiles = residual_ref.shape[0]
    pixels = table.shape[0] // ROWS

    def clear(number, carry):
        start = pl.multiple_of(number * 8 * ROWS, 8)
        table[pl.ds(start, 8 * ROWS), :] = jnp.zeros((8 * ROWS, 128), jnp.float32)
        return carry

    lax.fori_loop(0, pixels // 8, clear, 0)
    products[...] = jnp.zeros(products.shape, jnp.float32)
    lanes = lax.broadcasted_iota(jnp.int32, (SRC_PIX, 128), 0)

    def add_group(group, area):
        start = pl.multiple_of(group * GROUP, GROUP)
        rows = pl.ds(start, GROUP)
        weight = weight_ref[rows, :]
        baseline = residual_ref[rows, :]
        parts = [partial_ref[number, rows, :] for number in range(5)]
        scaled = [weight * part for part in parts]
        terms = [scaled[first] * parts[second] for first, second in SOURCE_PAIRS]
        terms = terms + [scaled[first] * baseline for first in range(5)]
        for number, term in enumerate(terms):
            products[pl.ds(area * GROUP * ROWS + number, GROUP, stride=ROWS), :] = term
        sums = []
        for tile in range(GROUP):
            full = products[pl.ds((area * GROUP + tile) * ROWS, ROWS), :]
            high = full.astype(jnp.bfloat16).astype(jnp.float32)
            both = jnp.concatenate([high, full - high], axis=0).astype(jnp.bfloat16)
            chosen = index_ref[pl.ds(start + tile, 1), :]
            hits = jnp.where(lanes == chosen, 1.0, 0.0).astype(jnp.bfloat16)
            spread = lax.dot_general(
                both, hits, (((1,), (1,)), ((), ())), preferred_element_type=jnp.float32
            )
            sums.append(spread[:ROWS] + spread[ROWS:])
        for tile in range(GROUP):
            slot = slot_ref[pixel_ref[start + tile]]
            place = pl.ds(pl.multiple_of(slot * ROWS, 8), ROWS)
            table[place, :] = table[place, :] + sums[tile]

    over_groups(tiles // GROUP, 4, add_group)

    me = me_ref[0]
    orders = halving_orders(sky, times)
    half = sky * times // 2
    length = bits_of(sky * times)
    for number, stage in enumerate(stages):
        chunk, sent = number // 2, number % 2
        order = orders[chunk % 4]

        def compact(place, carry):
            device = me ^ (sent << order[0])
            for at in range(1, length):
                device = device ^ (((place >> (length - 1 - at)) & 1) << order[at])
            base = (device % sky) * (share * times) + (device // sky) * share + chunk * 8
            for row in range(20):
                stage[place, row] = table[pl.ds(base * ROWS + row, 8, stride=ROWS), :]
            return carry

        lax.fori_loop(0, half, compact, 0)
        copy = pltpu.make_async_copy(stage, outs[number], done.at[number])
        copy.start()
        copies.append(copy)
    for copy in copies:
        copy.wait()


def local_normals(me, residual, weight, partials, index, tile_pixel, pixel_slot, sky, times):
    pixels = pixel_slot.shape[0]
    share = pixels // (sky * times)
    smem = pl.BlockSpec(memory_space=pltpu.SMEM)
    vmem = pl.BlockSpec(memory_space=pltpu.VMEM)
    return pl.pallas_call(
        functools.partial(normals_kernel, sky=sky, times=times, share=share),
        out_shape=[
            jax.ShapeDtypeStruct((sky * times // 2, 20, 8, 128), jnp.float32)
            for _ in range(share // 4)
        ],
        in_specs=[smem, smem, smem, vmem, vmem, vmem, vmem],
        out_specs=[pl.BlockSpec(memory_space=pl.ANY)] * (share // 4),
        scratch_shapes=[
            pltpu.VMEM((sky * times // 2, 20, 8, 128), jnp.float32) for _ in range(share // 4)
        ]
        + [
            pltpu.VMEM((pixels * ROWS, 128), jnp.float32),
            pltpu.VMEM((4 * GROUP * ROWS, 128), jnp.float32),
            pltpu.SemaphoreType.DMA((share // 4,)),
        ],
        compiler_params=pltpu.CompilerParams(vmem_limit_bytes=60000 * 1024),
        name="local_normals",
    )(me, pixel_slot, tile_pixel, residual, weight, partials, index)


def pair_kernel(weight_ref, attitude_ref, out_ref):
    lane = lax.broadcasted_iota(jnp.int32, (GROUP, 128), 1)

    def add_group(group, area):
        rows = pl.ds(pl.multiple_of(group * GROUP, GROUP), GROUP)
        weight = weight_ref[rows, :]
        result = jnp.zeros((GROUP, 128), jnp.float32)
        for segment in range(4):
            parts = [attitude_ref[4 * segment + number, rows, :] for number in range(4)]
            scaled = [weight * part for part in parts]
            for number, (first, second) in enumerate(KNOT_PAIRS):
                total = jnp.sum(scaled[first] * parts[second], axis=1, keepdims=True)
                result = jnp.where(lane == 16 * segment + number, total, result)
        out_ref[rows, :] = result

    over_groups(weight_ref.shape[0] // GROUP, 4, add_group)


def settle_kernel(
    base_ref, pixel_ref, residual_ref, weight_ref, partial_ref, index_ref, attitude_ref,
    pairs_ref, update_ref, settled_ref, out_ref, picked, *, part,
):
    block = residual_ref.shape[0]
    first_tile = pl.program_id(0) * block
    lane = lax.broadcasted_iota(jnp.int32, (GROUP, 128), 1)

    def add_group(group, area):
        start = pl.multiple_of(group * GROUP, GROUP)
        rows = pl.ds(start, GROUP)
        for tile in range(GROUP):
            base = base_ref[pixel_ref[first_tile + start + tile]]
            for number in range(5):
                picked[pl.ds((area * 5 + number) * GROUP + tile, 1), :] = update_ref[
                    pl.ds(base + number * part, 1), :
                ]
        index = index_ref[rows, :]
        total = None
        for number in range(5):
            values = jnp.take_along_axis(picked[pl.ds((area * 5 + number) * GROUP, GROUP), :], index, axis=1)
            addend = partial_ref[number, rows, :] * values
            total = addend if total is None else total + addend
        settled = residual_ref[rows, :] - total
        settled_ref[rows, :] = settled
        scaled = weight_ref[rows, :] * settled
        result = pairs_ref[rows, :]
        for segment in range(4):
            for number in range(4):
                amount = jnp.sum(
                    scaled * attitude_ref[4 * segment + number, rows, :], axis=1, keepdims=True
                )
                result = jnp.where(lane == 16 * segment + 10 + number, amount, result)
        out_ref[rows, :] = result

    over_groups(block // GROUP, 4, add_group)


def final_kernel(settled_ref, attitude_ref, values_ref, out_ref):
    def correct_group(group, area):
        rows = pl.ds(pl.multiple_of(group * GROUP, GROUP), GROUP)
        values = values_ref[rows, :]
        total = attitude_ref[0, rows, :] * values[:, 0:1]
        for number in range(1, 16):
            total = total + attitude_ref[number, rows, :] * values[:, number : number + 1]
        out_ref[rows, :] = settled_ref[rows, :] - total

    over_groups(settled_ref.shape[0] // GROUP, 4, correct_group)


def body(
    residual,
    obs_weight,
    source_partials,
    attitude_partials,
    source_index,
    tile_pixel,
    tile_knot,
    pixel_slot,
):
    sky = lax.axis_size("sky")
    times = lax.axis_size("tm")
    both = ("tm", "sky")
    devices = sky * times
    tiles = residual.shape[0]
    pixels = pixel_slot.shape[0]
    share = pixels // devices
    span = KNOTS_DEV // sky
    block = min(tiles, 128)
    steps = tiles // block
    smem = pl.BlockSpec(memory_space=pltpu.SMEM)
    flat = pl.BlockSpec((block, 128), lambda step: (step, 0))
    five = pl.BlockSpec((5, block, 128), lambda step: (0, step, 0))
    wide = pl.BlockSpec((16, block, 128), lambda step: (0, step, 0))
    flat_shape = jax.ShapeDtypeStruct((tiles, 128), jnp.float32)

    me = lax.axis_index(both)
    orders = halving_orders(sky, times)
    normals = local_normals(
        me[None], residual, obs_weight, source_partials, source_index, tile_pixel, pixel_slot,
        sky, times,
    )
    keeps, sends = list(normals[0::2]), list(normals[1::2])
    for step in range(bits_of(devices)):
        for chunk in range(len(keeps)):
            bit = orders[chunk % 4][step]
            arrived = swapped(sends[chunk], both, bit, devices)
            rest = keeps[chunk].shape[0] // 2
            if rest:
                sends[chunk] = keeps[chunk][rest:] + arrived[rest:]
                keeps[chunk] = keeps[chunk][:rest] + arrived[:rest]
            else:
                keeps[chunk] = keeps[chunk] + arrived
    summed = jnp.concatenate([keep[0] for keep in keeps], axis=1)
    pairs = pl.pallas_call(
        pair_kernel,
        grid=(steps,),
        out_shape=flat_shape,
        in_specs=[flat, wide],
        out_specs=flat,
        cost_estimate=pl.CostEstimate(
            flops=400 * tiles * 128 * 40, bytes_accessed=18 * tiles * 512, transcendentals=0
        ),
        name="knot_pairs",
    )(obs_weight, attitude_partials)
    update = damped_solve(summed[:15], summed[15:], 5, SOURCE_PAIRS)
    part = share // 2
    widths = [order[:0:-1] + [0] for order in orders[:2]]
    halves = []
    for side, order in enumerate(widths):
        held = update[None, :, side * part : (side + 1) * part]
        for bit in order:
            held = jnp.concatenate([held, swapped(held, both, bit, devices)], axis=0)
        halves.append(held)
    everything = jnp.concatenate([held.reshape(-1, SRC_PIX) for held in halves], axis=0)

    def spot(relative, order):
        place = 0
        for at, bit in enumerate(order):
            place = place + (((relative >> bit) & 1) << at)
        return place

    relative = me ^ ((pixel_slot // share) % times * sky + pixel_slot // (share * times))
    within = pixel_slot % share
    bases = [
        (side * devices + spot(relative, order)) * (5 * part) + within % part
        for side, order in enumerate(widths)
    ]
    base = jnp.where(within < part, bases[0], bases[1])
    time = lax.axis_index("tm")
    near = jnp.stack(
        [
            jnp.concatenate(
                [halves[side][spot(step * sky, widths[side])] for side in range(2)], axis=1
            )
            for step in range(times)
        ]
    )
    source_update = jnp.concatenate(
        [
            lax.dynamic_index_in_dim(near, time ^ step, 0, keepdims=False)
            for step in range(times)
        ],
        axis=1,
    ).reshape(5, times * share * SRC_PIX)
    settled, terms = pl.pallas_call(
        functools.partial(settle_kernel, part=part),
        grid=(steps,),
        out_shape=(flat_shape, flat_shape),
        in_specs=[
            smem, smem, flat, flat, five, flat, wide, flat,
            pl.BlockSpec((devices * 5 * share, 128), lambda step: (0, 0)),
        ],
        out_specs=(flat, flat),
        scratch_shapes=[pltpu.VMEM((4 * 5 * GROUP, 128), jnp.float32)],
        name="settle",
    )(
        base, tile_pixel, residual, obs_weight, source_partials, source_index,
        attitude_partials, pairs, everything,
    )
    start = tile_knot - me * span
    hits = (start[:, None] == jnp.arange(span, dtype=jnp.int32)[None, :]).astype(jnp.float32)
    sums = lax.dot_general(
        terms, hits, (((0,), (0,)), ((), ())), precision=lax.Precision.HIGHEST
    )
    local = sum(
        jnp.pad(sums[16 * segment : 16 * segment + 16], ((0, 0), (segment, 3 - segment)))
        for segment in range(4)
    )
    onward = [(device, device + 1) for device in range(devices - 1)]
    back = [(device + 1, device) for device in range(devices - 1)]
    arriving = lax.ppermute(local[:, span:], both, onward)
    whole = local[:, :span] + jnp.pad(arriving, ((0, 0), (0, span - 3)))
    own = damped_solve(whole[:10], whole[10:14], 4, KNOT_PAIRS)
    following = lax.ppermute(own[:, :3], both, back)
    extended = jnp.concatenate([own, following], axis=1)
    windows = jnp.concatenate([extended[:, segment : segment + span] for segment in range(4)])
    values = lax.dot_general(
        hits, windows, (((1,), (1,)), ((), ())), precision=lax.Precision.HIGHEST
    )
    late, values = lax.optimization_barrier((own, values))
    stacked = late[None]
    for bit in range(bits_of(sky)):
        stacked = jnp.concatenate([stacked, swapped(stacked, "sky", bit, sky)], axis=0)
    order = jnp.arange(sky, dtype=jnp.int32)
    turn = (order[:, None] ^ lax.axis_index("sky") == order[None, :]).astype(jnp.float32)
    attitude_update = jnp.einsum(
        "jr,rck->cjk", turn, stacked, precision=lax.Precision.HIGHEST
    ).reshape(4, sky * span)
    final_residual = pl.pallas_call(
        final_kernel,
        grid=(steps,),
        out_shape=flat_shape,
        in_specs=[flat, wide, pl.BlockSpec((block, 16), lambda step: (step, 0))],
        out_specs=flat,
        name="final",
    )(settled, attitude_partials, values)
    return (final_residual, source_update, attitude_update)


def solution(mesh):
    in_specs = (
        P(("tm", "sky"), None),
        P(("tm", "sky"), None),
        P(None, ("tm", "sky"), None),
        P(None, ("tm", "sky"), None),
        P(("tm", "sky"), None),
        P(("tm", "sky")),
        P(("tm", "sky")),
        P(),
    )
    out_specs = (P(("tm", "sky"), None), P(None, "sky"), P(None, "tm"))
    return jax.shard_map(body, mesh=mesh, in_specs=in_specs, out_specs=out_specs, check_vma=False)
```
